32 devices in a mesh: freq: 4 (over y, core), mesh: 8 (over z, x).
Axes of the slice: x: 2, y: 2, z: 4, core: 2. Of those that a mesh axis runs over, the one named last changes fastest.
Arguments:
- spectrum: float32 [2, 216, 32768], P(None, 'freq', 'mesh'), may hold values from -84 to 84
- time_weights: float32 [2, 432], P(None, 'freq'), may hold values from -0.625 to 0.625
- interp_weights: float32 [1024, 128, 128], P('mesh'), may hold values from -0.5 to 0.5
- group_block: int32 [1024], P('mesh'), may hold values from 0 to 255, as said below
- group_count: int32 [8], P('mesh'), may hold values from 64 to 128, as said below
- wave_state: float32 [4, 2, 524288], P('freq', None, 'mesh'), may hold values from -6 to 6
- neighbors: int32 [4, 4096], P(None, 'mesh'), may hold values from 0 to 575, as said below
- coupling: float32 [4, 524288], P(None, 'mesh'), may hold values from 0.02 to 0.2
Outputs:
- series: float32 [432, 32768], P('freq', 'mesh')
- new_state: float32 [4, 2, 524288], P('freq', None, 'mesh')
The draws below stay inside these ranges and needn't reach their ends.
Inputs may be any that keep to these rules, and one draw needn't show every extreme that they name: `group_block`: partition o owns blocks o * 32 to o * 32 + 31. Of one partition's 128 groups at most 16 name blocks of one owner, and each partition has an owner named by exactly 16 of its live groups. The live groups of partition m are its first group_count[m]; some partition has exactly 128. `neighbors`: for the cell row with local row index u, a value e names local row e - 32 of the row's own partition when it lies in 32 .. (69632) // 128 - 1, else a row of the neighbouring partition below or above; never the row itself.
All inputs are finite; a program needn't handle non-finite values.
Results may differ from the reference program's by a relative error of at most 0.0001.
Values sent between devices are 32-bit elements; how exact they have to be, the bound alone decides.
No kernel may reach another device: no remote copies, remote signals or barrier semaphores. Data moves between devices by JAX's collectives and lax.ppermute only.
A program may use at most 64 MiB of HBM per device.

```python
import math
import jax
import jax.numpy as jnp
from jax import lax

NF = 216
NT = 432
BS = 128
B_DEV = 32
NB = 256
NP = 32768
FG_MAX = 128
GROUPS = 1024
C_DEV = 65536
CELLS = 524288
LANES = 128
HB = 4096
NEIGH = 4
WINDOWS = 4
N_FREQ = 4
N_MESH = 8


def group_plan(base_key):
    count_key = jax.random.fold_in(base_key, 7)
    heaviest = jax.random.randint(jax.random.fold_in(count_key, 1), (), 0, N_MESH)
    lighter = jax.random.randint(jax.random.fold_in(count_key, 2), (N_MESH,), FG_MAX // 2, FG_MAX + 1)
    partitions = jnp.arange(N_MESH, dtype=jnp.int32)
    counts = jnp.where(partitions == heaviest, FG_MAX, lighter).astype(jnp.int32)
    capacity = max(2, FG_MAX // N_MESH)

    def one_partition(partition, live_count):
        partition_key = jax.random.fold_in(base_key, 1000 + partition)
        leading = jax.random.randint(jax.random.fold_in(partition_key, 1), (), 0, N_MESH).astype(jnp.int32)
        others = jax.random.permutation(jax.random.fold_in(partition_key, 2), (N_MESH - 1) * capacity) // capacity
        others = jnp.where(others >= leading, others + 1, others).astype(jnp.int32)
        owners = jnp.concatenate([jnp.full((capacity,), leading, jnp.int32), others])[:FG_MAX]
        positions = jnp.arange(FG_MAX, dtype=jnp.int32)
        ranking = jax.random.permutation(jax.random.fold_in(partition_key, 3), FG_MAX).astype(jnp.int32)
        scores = jnp.where(positions < live_count, ranking, FG_MAX + positions)
        ordering = jnp.argsort(scores, stable=True)
        owners = owners[ordering]
        inside = jax.random.randint(jax.random.fold_in(partition_key, 4), (FG_MAX,), 0, B_DEV)
        return (owners * B_DEV + inside).astype(jnp.int32)
    blocks = jax.vmap(one_partition)(partitions, counts)
    return (blocks.reshape(N_MESH * FG_MAX), counts)


def draw_group_block(key, part):
    return group_plan(key)[0]


def draw_group_count(key, part):
    return group_plan(key)[1]


def draw_neighbors(key, part):
    halo_rows = HB // LANES
    rows_local = C_DEV // LANES
    local_rows = jnp.arange(CELLS // LANES, dtype=jnp.int32) % rows_local
    offsets = jax.random.randint(jax.random.fold_in(key, 21), (NEIGH, CELLS // LANES), -halo_rows, halo_rows)
    offsets = jnp.where(offsets >= 0, offsets + 1, offsets)
    return (halo_rows + local_rows[None, :] + offsets).astype(jnp.int32)


def block_scale(key, shape, pieces, smallest, largest):
    gain, own = 1.0, jax.random.fold_in(key, 6)
    for dim, parts in pieces:
        heights = jnp.exp(jax.random.uniform(jax.random.fold_in(own, dim), (parts,), jnp.float32, smallest / len(pieces), largest / len(pieces)))
        gain = gain * jnp.repeat(heights, shape[dim] // parts).reshape([-1 if axis == dim else 1 for axis in range(len(shape))])
    return gain


def normal_values(own_key, extent, scale, bound, cuts=(), kind=jnp.bfloat16):
    result = scale * jax.random.normal(own_key, extent, jnp.float32)
    if cuts:
        result = result * block_scale(own_key, extent, cuts, -0.22, 0.18)
    return jnp.clip(result, -bound, bound).astype(kind)


def setup_inputs(seed: int = 0) -> dict:
    seeds = jax.random.split(jax.random.key(seed), 9)
    spectrum = normal_values(seeds[0], (2, NF, NP), 14.0, 84.0, ((1, 4), (2, 8)), jnp.float32)
    time_weights = normal_values(seeds[1], (2, NT), (NT // N_FREQ) ** -0.5, 0.625, ((1, 4),), jnp.float32)
    interp_weights = normal_values(seeds[2], (GROUPS, BS, BS), BS ** -0.5, 0.5, ((0, 8),), jnp.float32)
    group_block = draw_group_block(jax.random.fold_in(seeds[8], 71), 0)
    group_count = draw_group_count(jax.random.fold_in(seeds[8], 71), 0)
    wave_state = normal_values(seeds[5], (WINDOWS, 2, CELLS), 1.0, 6.0, ((0, 4), (2, 8)), jnp.float32)
    neighbors = draw_neighbors(jax.random.fold_in(seeds[8], 71), 0)
    coupling = jnp.clip(jnp.exp(math.log(0.2) - 2.3025851 * jax.random.uniform(seeds[7], (NEIGH, CELLS), jnp.float32) ** block_scale(seeds[7], (NEIGH, CELLS), ((1, 8),), -0.2, 0.2)), 0.02, 0.2)
    return dict(spectrum=spectrum, time_weights=time_weights, interp_weights=interp_weights, group_block=group_block, group_count=group_count, wave_state=wave_state, neighbors=neighbors, coupling=coupling)


highest = lax.Precision.HIGHEST


def advance(previous, current, forcing, neighbors, coupling):
    halo_rows = HB // LANES
    row_count = CELLS // LANES
    rows_local = C_DEV // LANES
    cell_rows = current.reshape(row_count, LANES)
    extended = jnp.pad(cell_rows, ((halo_rows, halo_rows), (0, 0)))
    offsets = (jnp.arange(row_count, dtype=jnp.int32) // rows_local) * rows_local
    beside_all = extended[offsets[None, :] + neighbors].reshape(NEIGH, CELLS)
    spread = jnp.sum(coupling * (beside_all - current[None, :]), axis=0)
    return 2.0 * current - previous + spread + forcing


def reference(spectrum, time_weights, interp_weights, group_block, group_count, wave_state, neighbors, coupling):
    time_horizon = 2 * NF
    sample_times = jnp.arange(time_horizon, dtype=jnp.int32)
    angular_frequency = jnp.arange(NF, dtype=jnp.int32)
    phase_angles = ((sample_times[:, None] * angular_frequency[None, :]) % time_horizon).astype(jnp.float32)
    angles = phase_angles * (2.0 * math.pi / time_horizon)
    scales = jnp.where(angular_frequency == 0, 1.0, 2.0).astype(jnp.float32) / time_horizon
    basis_row_matrix = jnp.concatenate([jnp.cos(angles) * scales, -jnp.sin(angles) * scales], axis=1)
    series = jnp.dot(basis_row_matrix, spectrum.reshape(2 * NF, NP), precision=highest, preferred_element_type=jnp.float32)
    taper_window = time_horizon // N_FREQ
    live_mask = (jnp.arange(FG_MAX, dtype=jnp.int32)[None, :] < group_count[:, None]).reshape(GROUPS).astype(jnp.float32)
    blocks = series.reshape(time_horizon, NB, BS)
    states = []
    for window_index in range(N_FREQ):
        picked = blocks[window_index * taper_window:(window_index + 1) * taper_window][:, group_block, :]
        interpolated = jnp.einsum("rgp,gfp->rgf", picked, interp_weights, precision=highest)
        interpolated = interpolated * live_mask[None, :, None]
        weights_here = time_weights[:, window_index * taper_window:(window_index + 1) * taper_window]
        forcing = jnp.einsum("sr,rgf->sgf", weights_here, interpolated, precision=highest)
        forcing = forcing.reshape(2, N_MESH, FG_MAX * BS)
        forcing = jnp.pad(forcing, ((0, 0), (0, 0), (0, C_DEV - FG_MAX * BS))).reshape(2, CELLS)
        previous = wave_state[window_index, 0]
        current = wave_state[window_index, 1]
        stepped = advance(previous, current, forcing[0], neighbors, coupling)
        stepped_again = advance(current, stepped, forcing[1], neighbors, coupling)
        states.append(jnp.stack([stepped, stepped_again]))
    return series, jnp.stack(states)
```

```python
import math

import jax
import jax.numpy as jnp
from jax import lax
from jax.experimental import pallas as pl
from jax.experimental.pallas import tpu as pltpu
from jax.sharding import PartitionSpec as P

HB = 4096

high = lax.Precision.HIGH


def trig(times, freqs, horizon):
    phase = (times[:, None] * freqs[None, :] % horizon).astype(jnp.float32)
    angles = phase * (2.0 * math.pi / horizon)
    scales = jnp.where(freqs == 0, 1.0, 2.0).astype(jnp.float32) / horizon
    return jnp.cos(angles) * scales, -jnp.sin(angles) * scales


def mm(a, b):
    return jnp.dot(a, b, precision=high, preferred_element_type=jnp.float32)


def spread_rows(nbr_ref, coup_ref, ext_ref, got_ref, rows):
    faces = coup_ref.shape[0]
    unroll = 8

    def body(i, carry):
        for j in range(unroll):
            u = i * unroll + j
            for n in range(faces):
                got_ref[n, pl.ds(u, 1), :] = ext_ref[pl.ds(nbr_ref[n, u], 1), :]
        return carry

    lax.fori_loop(0, rows // unroll, body, 0)


def first_kernel(nbr_ref, low_ref, high_ref, state_ref, coup_ref, out_ref, ext_ref, got_ref):
    rows = state_ref.shape[1]
    halo = low_ref.shape[0]
    ext_ref[pl.ds(0, halo), :] = low_ref[...]
    ext_ref[pl.ds(halo, rows), :] = state_ref[1]
    ext_ref[pl.ds(halo + rows, halo), :] = high_ref[...]
    spread_rows(nbr_ref, coup_ref, ext_ref, got_ref, rows)
    cur = state_ref[1]
    total = 2.0 * cur - state_ref[0]
    for n in range(coup_ref.shape[0]):
        total = total + coup_ref[n] * (got_ref[n] - cur)
    out_ref[...] = total


def second_kernel(
    nbr_ref, low_ref, high_ref, base_ref, prev_ref, push_ref, coup_ref, out_ref, ext_ref, got_ref
):
    rows = base_ref.shape[0]
    halo = low_ref.shape[0]
    groups = push_ref.shape[1]
    ext_ref[pl.ds(0, halo), :] = low_ref[...]
    ext_ref[pl.ds(halo, rows), :] = base_ref[...]
    ext_ref[pl.ds(halo, groups), :] = base_ref[pl.ds(0, groups), :] + push_ref[0]
    ext_ref[pl.ds(halo + rows, halo), :] = high_ref[...]
    spread_rows(nbr_ref, coup_ref, ext_ref, got_ref, rows)
    cur = ext_ref[pl.ds(halo, rows), :]
    out_ref[0] = cur
    total = 2.0 * cur - prev_ref[...]
    for n in range(coup_ref.shape[0]):
        total = total + coup_ref[n] * (got_ref[n] - cur)
    out_ref[1] = total
    out_ref[1, pl.ds(0, groups), :] = out_ref[1, pl.ds(0, groups), :] + push_ref[1]


def call(kernel, out_shape, rows, lanes, halo, faces, args):
    vmem = pl.BlockSpec(memory_space=pltpu.VMEM)
    smem = pl.BlockSpec(memory_space=pltpu.SMEM)
    return pl.pallas_call(
        kernel,
        out_shape=jax.ShapeDtypeStruct(out_shape, jnp.float32),
        in_specs=[smem] + [vmem] * (len(args) - 1),
        out_specs=vmem,
        scratch_shapes=[
            pltpu.VMEM((rows + 2 * halo, lanes), jnp.float32),
            pltpu.VMEM((faces, rows, lanes), jnp.float32),
        ],
    )(*args)


def local(
    spectrum,
    time_weights,
    interp_weights,
    group_block,
    group_count,
    wave_state,
    neighbors,
    coupling,
):
    parts, local_freqs, points = spectrum.shape
    nf = lax.axis_size("freq")
    nm = lax.axis_size("mesh")
    me = lax.axis_index("freq")
    horizon = 2 * local_freqs * nf
    window = horizon // nf
    cores = 2 if nf % 2 == 0 else 1
    chips = nf // cores

    def across(x, d):
        return lax.ppermute(x, "freq", [(i, (i + d * cores) % nf) for i in range(nf)])

    def beside(x):
        return lax.ppermute(x, "freq", [(i, i ^ 1) for i in range(nf)])

    own = [spectrum[p] for p in range(parts)]
    far = [(d, p, across(own[p], d)) for d in range(1, chips) for p in range(parts)]
    pieces_near = [(me, p, own[p]) for p in range(parts)]
    pieces_far = [((me - d * cores) % nf, p, x) for d, p, x in far]
    if cores == 2:
        mate = beside(spectrum)
        pieces_near += [(me ^ 1, p, mate[p]) for p in range(parts)]
        pieces_far += [(((me ^ 1) - d * cores) % nf, p, beside(x)) for d, p, x in far]

    groups, block = interp_weights.shape[:2]
    faces, rows = neighbors.shape
    lanes = wave_state.shape[2] // rows
    halo = HB // lanes
    up = [(i, i + 1) for i in range(nm - 1)]
    down = [(i + 1, i) for i in range(nm - 1)]
    state = wave_state.reshape(2, rows, lanes)
    coup = coupling.reshape(faces, rows, lanes)
    low0 = lax.ppermute(state[1, rows - halo :], "mesh", up)
    high0 = lax.ppermute(state[1, :halo], "mesh", down)

    weights = lax.all_gather(time_weights, "freq", axis=0)
    times = lax.iota(jnp.int32, horizon)
    cos_own, sin_own = trig(times, me * local_freqs + lax.iota(jnp.int32, local_freqs), horizon)
    basis_own = jnp.concatenate([cos_own, sin_own], axis=1).reshape(nf, window, 2 * local_freqs)
    folded = jnp.einsum(
        "wsr,wrk->wsk", weights, basis_own, precision=lax.Precision.HIGHEST
    ).reshape(nf * 2, 2 * local_freqs)
    partial = mm(folded[:, :local_freqs], own[0]) + mm(folded[:, local_freqs:], own[1])
    per_owner = points // block
    partial = partial.reshape(nf, 2 * per_owner, block)
    weighted = jnp.sum(
        lax.all_to_all(partial, "freq", split_axis=0, concat_axis=0, tiled=True), axis=0
    )
    table = lax.all_gather(weighted, "mesh", axis=0, tiled=True)

    base = call(
        first_kernel, (rows, lanes), rows, lanes, halo, faces,
        (neighbors, low0, high0, state, coup),
    )

    owner = group_block // per_owner
    index = owner * (2 * per_owner) + group_block % per_owner
    live = (lax.iota(jnp.int32, groups) < group_count[0]).astype(jnp.float32)
    index = jnp.concatenate([index, index + per_owner])
    picked = table.at[index].get(mode="promise_in_bounds").reshape(2, groups, block)
    picked = picked * live[None, :, None]
    push = jnp.einsum("rgp,gfp->rgf", picked, interp_weights, precision=high)

    edge = base[:halo] + push[0, :halo]
    high1 = lax.ppermute(edge, "mesh", down)
    low1 = lax.ppermute(base[rows - halo :], "mesh", up)
    new_state = call(
        second_kernel, (2, rows, lanes), rows, lanes, halo, faces,
        (neighbors, low1, high1, base, state[1], push, coup),
    ).reshape(1, 2, rows * lanes)

    my_times = me * window + lax.iota(jnp.int32, window)

    def build(pieces):
        mats, blocks = [], []
        for source, part, x in pieces:
            freqs = source * local_freqs + lax.iota(jnp.int32, local_freqs)
            mats.append(trig(my_times, freqs, horizon)[part])
            blocks.append(x)
        return mm(jnp.concatenate(mats, axis=1), jnp.concatenate(blocks, axis=0))

    series = build(pieces_near)
    if pieces_far:
        series = series + build(pieces_far)
    return (series, new_state)


def solution(mesh):
    placed = (
        P(None, "freq", "mesh"),
        P(None, "freq"),
        P("mesh", None, None),
        P("mesh"),
        P("mesh"),
        P("freq", None, "mesh"),
        P(None, "mesh"),
        P(None, "mesh"),
    )
    return jax.shard_map(
        local,
        mesh=mesh,
        in_specs=placed,
        out_specs=(P("freq", "mesh"), P("freq", None, "mesh")),
        check_vma=False,
    )
```

```python
import math

import jax
import jax.numpy as jnp
from jax import lax
from jax.experimental import pallas as pl
from jax.experimental.pallas import tpu as pltpu
from jax.sharding import PartitionSpec as P


HB = 4096

high = lax.Precision.HIGH


def basis(times, first, count, horizon):
    column = lax.iota(jnp.int32, 2 * count)
    freqs = first + column // 2
    phase = (times[:, None] * freqs[None, :] % horizon).astype(jnp.float32)
    angles = phase * (2.0 * math.pi / horizon)
    scales = jnp.where(freqs == 0, 1.0, 2.0).astype(jnp.float32) / horizon
    return jnp.where(column % 2 == 0, jnp.cos(angles), -jnp.sin(angles)) * scales


def mm(a, b):
    return jnp.dot(a, b, precision=high, preferred_element_type=jnp.float32)


def spread_rows(nbr_ref, coup_ref, ext_ref, got_ref, rows):
    faces = coup_ref.shape[0]
    unroll = 8

    def body(i, carry):
        for j in range(unroll):
            u = i * unroll + j
            for n in range(faces):
                got_ref[n, pl.ds(u, 1), :] = ext_ref[pl.ds(nbr_ref[n, u], 1), :]
        return carry

    lax.fori_loop(0, rows // unroll, body, 0)


def first_kernel(nbr_ref, low_ref, high_ref, state_ref, coup_ref, out_ref, ext_ref, got_ref):
    rows = state_ref.shape[1]
    halo = low_ref.shape[0]
    ext_ref[pl.ds(0, halo), :] = low_ref[...]
    ext_ref[pl.ds(halo, rows), :] = state_ref[1]
    ext_ref[pl.ds(halo + rows, halo), :] = high_ref[...]
    spread_rows(nbr_ref, coup_ref, ext_ref, got_ref, rows)
    cur = state_ref[1]
    total = 2.0 * cur - state_ref[0]
    for n in range(coup_ref.shape[0]):
        total = total + coup_ref[n] * (got_ref[n] - cur)
    out_ref[...] = total


def second_kernel(
    nbr_ref, low_ref, high_ref, base_ref, prev_ref, push_ref, coup_ref, out_ref, ext_ref, got_ref
):
    rows = base_ref.shape[0]
    halo = low_ref.shape[0]
    groups = push_ref.shape[1]
    ext_ref[pl.ds(0, halo), :] = low_ref[...]
    ext_ref[pl.ds(halo, rows), :] = base_ref[...]
    ext_ref[pl.ds(halo, groups), :] = base_ref[pl.ds(0, groups), :] + push_ref[0]
    ext_ref[pl.ds(halo + rows, halo), :] = high_ref[...]
    spread_rows(nbr_ref, coup_ref, ext_ref, got_ref, rows)
    cur = ext_ref[pl.ds(halo, rows), :]
    out_ref[0] = cur
    total = 2.0 * cur - prev_ref[...]
    for n in range(coup_ref.shape[0]):
        total = total + coup_ref[n] * (got_ref[n] - cur)
    out_ref[1] = total
    out_ref[1, pl.ds(0, groups), :] = out_ref[1, pl.ds(0, groups), :] + push_ref[1]


def call(kernel, out_shape, rows, lanes, halo, faces, args):
    vmem = pl.BlockSpec(memory_space=pltpu.VMEM)
    smem = pl.BlockSpec(memory_space=pltpu.SMEM)
    return pl.pallas_call(
        kernel,
        out_shape=jax.ShapeDtypeStruct(out_shape, jnp.float32),
        in_specs=[smem] + [vmem] * (len(args) - 1),
        out_specs=vmem,
        scratch_shapes=[
            pltpu.VMEM((rows + 2 * halo, lanes), jnp.float32),
            pltpu.VMEM((faces, rows, lanes), jnp.float32),
        ],
    )(*args)


def body(
    spectrum,
    time_weights,
    interp_weights,
    group_block,
    group_count,
    wave_state,
    neighbors,
    coupling,
):
    parts, local_freqs, points = spectrum.shape
    nf = lax.axis_size("freq")
    nm = lax.axis_size("mesh")
    me = lax.axis_index("freq")
    horizon = 2 * local_freqs * nf
    window = horizon // nf
    cores = 2 if nf % 2 == 0 else 1
    chips = nf // cores

    def across(x, d):
        return lax.ppermute(x, "freq", [(i, (i + d * cores) % nf) for i in range(nf)])

    def beside(x):
        return lax.ppermute(x, "freq", [(i, i ^ 1) for i in range(nf)])

    width = parts * local_freqs
    stacked = jnp.transpose(spectrum, (1, 0, 2)).reshape(width, points)
    step = max(8, -(-3 * width // 8) // 8 * 8)
    cuts = [(at, min(at + step, width)) for at in range(0, width, step)]

    groups, block = interp_weights.shape[:2]
    faces, rows = neighbors.shape
    lanes = wave_state.shape[2] // rows
    halo = HB // lanes
    up = [(i, i + 1) for i in range(nm - 1)]
    down = [(i + 1, i) for i in range(nm - 1)]
    state = wave_state.reshape(2, rows, lanes)
    coup = coupling.reshape(faces, rows, lanes)
    low0 = lax.ppermute(state[1, rows - halo :], "mesh", up)
    high0 = lax.ppermute(state[1, :halo], "mesh", down)

    weights = lax.all_gather(time_weights, "freq", axis=0)
    times = lax.iota(jnp.int32, horizon)
    basis_own = basis(times, me * local_freqs, local_freqs, horizon).reshape(nf, window, width)
    folded = jnp.einsum(
        "wsr,wrk->wsk", weights, basis_own, precision=lax.Precision.HIGHEST
    ).reshape(nf * 2, width)
    weights, stacked = lax.optimization_barrier((weights, stacked))
    mate = beside(stacked) if cores == 2 else None
    head = [across(stacked[slice(*cuts[0])], d) for d in range(1, chips)]
    partial = mm(folded, stacked)
    per_owner = points // block
    partial = partial.reshape(nf, 2 * per_owner, block)
    weighted = jnp.sum(
        lax.all_to_all(partial, "freq", split_axis=0, concat_axis=0, tiled=True), axis=0
    )
    table = lax.all_gather(weighted, "mesh", axis=0, tiled=True)
    table, stacked_late = lax.optimization_barrier((table, stacked))
    tails = [
        [across(stacked_late[slice(*cut)], d) for d in range(1, chips)] for cut in cuts[1:]
    ]

    base = call(
        first_kernel, (rows, lanes), rows, lanes, halo, faces,
        (neighbors, low0, high0, state, coup),
    )

    owner = group_block // per_owner
    index = owner * (2 * per_owner) + group_block % per_owner
    live = (lax.iota(jnp.int32, groups) < group_count[0]).astype(jnp.float32)
    index = jnp.concatenate([index, index + per_owner])
    picked = table.at[index].get(mode="promise_in_bounds").reshape(2, groups, block)
    picked = picked * live[None, :, None]
    push = jnp.einsum("rgp,gfp->rgf", picked, interp_weights, precision=high)

    edge = base[:halo] + push[0, :halo]
    high1 = lax.ppermute(edge, "mesh", down)
    low1 = lax.ppermute(base[rows - halo :], "mesh", up)
    new_state = call(
        second_kernel, (2, rows, lanes), rows, lanes, halo, faces,
        (neighbors, low1, high1, base, state[1], push, coup),
    )
    if tails:
        new_state, tails[-1] = lax.optimization_barrier((new_state, tails[-1]))
    new_state = new_state.reshape(1, 2, rows * lanes)

    my_times = me * window + lax.iota(jnp.int32, window)

    def table_of(source):
        return basis(my_times, source * local_freqs, local_freqs, horizon)

    series = mm(table_of(me), stacked)
    if cores == 2:
        series = series + mm(table_of(me ^ 1), mate)
    far = [(me - d * cores) % nf for d in range(1, chips)]
    far_tables = [(table_of(f), table_of(f ^ 1)) for f in far]
    for cut, arrived in zip(cuts, [head] + tails):
        for (here, there), x in zip(far_tables, arrived):
            if cores == 2:
                passed = beside(x)
                series = series + mm(here[:, slice(*cut)], x)
                series = series + mm(there[:, slice(*cut)], passed)
            else:
                series = series + mm(here[:, slice(*cut)], x)
    return (series, new_state)


def solution(mesh):
    placed = (
        P(None, "freq", "mesh"),
        P(None, "freq"),
        P("mesh", None, None),
        P("mesh"),
        P("mesh"),
        P("freq", None, "mesh"),
        P(None, "mesh"),
        P(None, "mesh"),
    )
    return jax.shard_map(
        body,
        mesh=mesh,
        in_specs=placed,
        out_specs=(P("freq", "mesh"), P("freq", None, "mesh")),
        check_vma=False,
    )
```

```python
import math

import jax
import jax.numpy as jnp
from jax import lax
from jax.experimental import pallas as pl
from jax.experimental.pallas import tpu as pltpu
from jax.sharding import PartitionSpec as P


HB = 4096

high = lax.Precision.HIGH


def basis(times, first, count, horizon):
    column = lax.iota(jnp.int32, 2 * count)
    freqs = first + column // 2
    phase = (times[:, None] * freqs[None, :] % horizon).astype(jnp.float32)
    angles = phase * (2.0 * math.pi / horizon)
    scales = jnp.where(freqs == 0, 1.0, 2.0).astype(jnp.float32) / horizon
    return jnp.where(column % 2 == 0, jnp.cos(angles), -jnp.sin(angles)) * scales


def mm(a, b):
    return jnp.dot(a, b, precision=high, preferred_element_type=jnp.float32)


def spread_rows(nbr_ref, coup_ref, ext_ref, got_ref, rows):
    faces = coup_ref.shape[0]
    unroll = 8

    def body(i, carry):
        for j in range(unroll):
            u = i * unroll + j
            for n in range(faces):
                got_ref[n, pl.ds(u, 1), :] = ext_ref[pl.ds(nbr_ref[n, u], 1), :]
        return carry

    lax.fori_loop(0, rows // unroll, body, 0)


def first_kernel(nbr_ref, low_ref, high_ref, state_ref, coup_ref, out_ref, ext_ref, got_ref):
    rows = state_ref.shape[1]
    halo = low_ref.shape[0]
    ext_ref[pl.ds(0, halo), :] = low_ref[...]
    ext_ref[pl.ds(halo, rows), :] = state_ref[1]
    ext_ref[pl.ds(halo + rows, halo), :] = high_ref[...]
    spread_rows(nbr_ref, coup_ref, ext_ref, got_ref, rows)
    cur = state_ref[1]
    total = 2.0 * cur - state_ref[0]
    for n in range(coup_ref.shape[0]):
        total = total + coup_ref[n] * (got_ref[n] - cur)
    out_ref[...] = total


def second_kernel(
    nbr_ref, low_ref, high_ref, base_ref, prev_ref, push_ref, coup_ref, out_ref, ext_ref, got_ref
):
    rows = base_ref.shape[0]
    halo = low_ref.shape[0]
    groups = push_ref.shape[1]
    ext_ref[pl.ds(0, halo), :] = low_ref[...]
    ext_ref[pl.ds(halo, rows), :] = base_ref[...]
    ext_ref[pl.ds(halo, groups), :] = base_ref[pl.ds(0, groups), :] + push_ref[0]
    ext_ref[pl.ds(halo + rows, halo), :] = high_ref[...]
    spread_rows(nbr_ref, coup_ref, ext_ref, got_ref, rows)
    cur = ext_ref[pl.ds(halo, rows), :]
    out_ref[0] = cur
    total = 2.0 * cur - prev_ref[...]
    for n in range(coup_ref.shape[0]):
        total = total + coup_ref[n] * (got_ref[n] - cur)
    out_ref[1] = total
    out_ref[1, pl.ds(0, groups), :] = out_ref[1, pl.ds(0, groups), :] + push_ref[1]


def call(kernel, out_shape, rows, lanes, halo, faces, args):
    vmem = pl.BlockSpec(memory_space=pltpu.VMEM)
    smem = pl.BlockSpec(memory_space=pltpu.SMEM)
    return pl.pallas_call(
        kernel,
        out_shape=jax.ShapeDtypeStruct(out_shape, jnp.float32),
        in_specs=[smem] + [vmem] * (len(args) - 1),
        out_specs=vmem,
        scratch_shapes=[
            pltpu.VMEM((rows + 2 * halo, lanes), jnp.float32),
            pltpu.VMEM((faces, rows, lanes), jnp.float32),
        ],
    )(*args)


def body(
    spectrum,
    time_weights,
    interp_weights,
    group_block,
    group_count,
    wave_state,
    neighbors,
    coupling,
):
    parts, local_freqs, points = spectrum.shape
    nf = lax.axis_size("freq")
    nm = lax.axis_size("mesh")
    me = lax.axis_index("freq")
    horizon = 2 * local_freqs * nf
    window = horizon // nf
    cores = 2 if nf % 2 == 0 else 1
    chips = nf // cores

    def across(x, d):
        return lax.ppermute(x, "freq", [(i, (i + d * cores) % nf) for i in range(nf)])

    def beside(x):
        return lax.ppermute(x, "freq", [(i, i ^ 1) for i in range(nf)])

    width = parts * local_freqs
    stacked = jnp.transpose(spectrum, (1, 0, 2)).reshape(width, points)
    step = max(8, -(-7 * width // 16) // 8 * 8)
    cuts = [(0, step), (step, width)]

    groups, block = interp_weights.shape[:2]
    faces, rows = neighbors.shape
    lanes = wave_state.shape[2] // rows
    halo = HB // lanes
    up = [(i, i + 1) for i in range(nm - 1)]
    down = [(i + 1, i) for i in range(nm - 1)]
    state = wave_state.reshape(2, rows, lanes)
    coup = coupling.reshape(faces, rows, lanes)
    low0 = lax.ppermute(state[1, rows - halo :], "mesh", up)
    high0 = lax.ppermute(state[1, :halo], "mesh", down)

    weights = lax.all_gather(time_weights, "freq", axis=0)
    times = lax.iota(jnp.int32, horizon)
    basis_own = basis(times, me * local_freqs, local_freqs, horizon).reshape(nf, window, width)
    folded = jnp.einsum(
        "wsr,wrk->wsk", weights, basis_own, precision=lax.Precision.HIGHEST
    ).reshape(nf * 2, width)
    weights, stacked = lax.optimization_barrier((weights, stacked))
    mate = beside(stacked) if cores == 2 else None
    head = [across(stacked[slice(*cuts[0])], d) for d in range(1, chips)]
    partial = mm(folded, stacked)
    per_owner = points // block
    partial = partial.reshape(nf, 2 * per_owner, block)
    weighted = jnp.sum(
        lax.all_to_all(partial, "freq", split_axis=0, concat_axis=0, tiled=True), axis=0
    )
    table = lax.all_to_all(
        jnp.broadcast_to(weighted, (nm, *weighted.shape)),
        "mesh", split_axis=0, concat_axis=0, tiled=True,
    ).reshape(nm * weighted.shape[0], block)

    base = call(
        first_kernel, (rows, lanes), rows, lanes, halo, faces,
        (neighbors, low0, high0, state, coup),
    )

    head, stacked_late, base = lax.optimization_barrier((head, stacked, base))
    tails = [[across(stacked_late[slice(*cuts[1])], d) for d in range(1, chips)]]

    owner = group_block // per_owner
    index = owner * (2 * per_owner) + group_block % per_owner
    live = (lax.iota(jnp.int32, groups) < group_count[0]).astype(jnp.float32)
    index = jnp.concatenate([index, index + per_owner])
    picked = table.at[index].get(mode="promise_in_bounds").reshape(2, groups, block)
    picked = picked * live[None, :, None]
    push = jnp.einsum("rgp,gfp->rgf", picked, interp_weights, precision=high)

    edge = base[:halo] + push[0, :halo]
    high1 = lax.ppermute(edge, "mesh", down)
    low1 = lax.ppermute(base[rows - halo :], "mesh", up)
    new_state = call(
        second_kernel, (2, rows, lanes), rows, lanes, halo, faces,
        (neighbors, low1, high1, base, state[1], push, coup),
    )
    if tails:
        new_state, tails[-1] = lax.optimization_barrier((new_state, tails[-1]))
    new_state = new_state.reshape(1, 2, rows * lanes)

    my_times = me * window + lax.iota(jnp.int32, window)

    def table_of(source):
        return basis(my_times, source * local_freqs, local_freqs, horizon)

    series = mm(table_of(me), stacked)
    if cores == 2:
        series = series + mm(table_of(me ^ 1), mate)
    far = [(me - d * cores) % nf for d in range(1, chips)]
    far_tables = [(table_of(f), table_of(f ^ 1)) for f in far]
    for cut, arrived in zip(cuts, [head] + tails):
        for (here, there), x in zip(far_tables, arrived):
            if cores == 2:
                passed = beside(x)
                series = series + mm(here[:, slice(*cut)], x)
                series = series + mm(there[:, slice(*cut)], passed)
            else:
                series = series + mm(here[:, slice(*cut)], x)
    return (series, new_state)


def solution(mesh):
    placed = (
        P(None, "freq", "mesh"),
        P(None, "freq"),
        P("mesh", None, None),
        P("mesh"),
        P("mesh"),
        P("freq", None, "mesh"),
        P(None, "mesh"),
        P(None, "mesh"),
    )
    return jax.shard_map(
        body,
        mesh=mesh,
        in_specs=placed,
        out_specs=(P("freq", "mesh"), P("freq", None, "mesh")),
        check_vma=False,
    )
```
